128 devices in a mesh: basin: 16 (over y, x), tile: 8 (over z, core).
Axes of the slice: x: 4, y: 4, z: 4, core: 2. Of those that a mesh axis runs over, the one named last changes fastest.
Arguments:
- tile_water: float32 [16, 128, 4096], P('basin', None, 'tile'), may hold values from 0.1 to 3
- tile_frac: float32 [16, 128, 4096], P('basin', None, 'tile'), may hold values from 0.01 to 0.12
- tile_cell: int32 [16, 128, 4096], P('basin', None, 'tile'), may hold values from 0 to 255
- storage: float32 [16, 128, 256], P('basin', 'tile'), may hold values from 0 to 2
- kappa: float32 [16, 128, 256], P('basin', 'tile'), may hold values from 0.4 to 1
- inverse: float32 [16, 128, 256, 256], P('basin', 'tile'), may hold values from -0.25 to 1.15
- cell_mask: int32 [16, 128, 256], P('basin', 'tile'), may hold values 0 or 1
- upstream: int32 [16, 128], P('basin', 'tile'), may hold values from 0 to 15, as said below
Outputs:
- level: float32 [16, 128, 256], P('basin', 'tile')
- discharge: float32 [16, 128, 256], P('basin', 'tile')
The draws below stay inside these ranges and needn't reach their ends.
Inputs may be any that keep to these rules, and one draw needn't show every extreme that they name: `upstream`: for each reach position and each group of 16 consecutive chains, the values form a permutation of 0 to 15.
All inputs are finite; a program needn't handle non-finite values. No bound on the sum of `cell_mask` on one device may be relied on, other than what follows from the above.
Results may differ from the reference program's by a relative error of at most 0.0001.
Values sent between devices are 32-bit elements; how exact they have to be, the bound alone decides.
No kernel may reach another device: no remote copies, remote signals or barrier semaphores. Data moves between devices by JAX's collectives and lax.ppermute only.
A program may use at most 64 MiB of HBM per device.

```python
import math
import jax
import jax.numpy as jnp
from jax import lax

BLOCK = 256
CH_DEV = 16
SUBSTEPS = 3
CHAINS = 128
POSITIONS = 16
TPB = 4096


def draw_inverse(key, part):
    shape = (POSITIONS, CHAINS, BLOCK, BLOCK)
    noise = jnp.clip(jax.random.normal(key, shape, jnp.float32), -4.0, 4.0) * (0.3 / BLOCK ** 0.5)
    return noise + 0.9 * jnp.eye(BLOCK, dtype=jnp.float32)


def draw_upstream(key, part):
    keys = jax.random.split(jax.random.fold_in(key, 7), POSITIONS * (CHAINS // CH_DEV))
    perms = jax.vmap(lambda single: jax.random.permutation(single, CH_DEV))(keys)
    return perms.reshape(POSITIONS, CHAINS).astype(jnp.int32)


def plant(values, stream_key, least, high):
    longest = values.shape.index(max(values.shape))
    spots = []
    for shift in (0, 1):
        where = [jax.random.randint(jax.random.fold_in(stream_key, axis), (), 0, length) for axis, length in enumerate(values.shape)]
        where[longest] = (where[longest] + shift) % values.shape[longest]
        spots.append(tuple(where))
    return values.at[spots[0]].set(least).at[spots[1]].set(high)


def shard_levels(stream_key, extent, shards, least, largest):
    def one(axis_at, shards_of):
        steps = jax.random.uniform(jax.random.fold_in(jax.random.fold_in(stream_key, 6), axis_at), (shards_of,), jnp.float32, least / len(shards), largest / len(shards))
        return jnp.repeat(jnp.exp(steps), extent[axis_at] // shards_of).reshape((-1,) + (1,) * (len(extent) - axis_at - 1))

    level = one(*shards[0])
    for cut in shards[1:]:
        level = level * one(*cut)
    return level


def setup_inputs(seed: int = 0) -> dict:
    streams_of = jax.random.split(jax.random.key(seed), 9)
    return {
        "tile_water": jnp.clip(jnp.exp(math.log(3.0) - 3.4011974 * jax.random.uniform(streams_of[0], (POSITIONS, CHAINS, TPB), jnp.float32) ** shard_levels(streams_of[0], (POSITIONS, CHAINS, TPB), ((0, 16), (2, 8)), -0.2, 0.2)), 0.1, 3.0),
        "tile_frac": jnp.clip(jnp.exp(math.log(0.12) - 2.4849066 * jax.random.uniform(streams_of[1], (POSITIONS, CHAINS, TPB), jnp.float32) ** shard_levels(streams_of[1], (POSITIONS, CHAINS, TPB), ((0, 16), (2, 8)), -0.2, 0.2)), 0.01, 0.12),
        "tile_cell": plant(jax.random.randint(streams_of[2], (POSITIONS, CHAINS, TPB), 0, BLOCK), jax.random.fold_in(streams_of[2], 1), 0, BLOCK - 1).astype(jnp.int32),
        "storage": jnp.clip(2.0 * jax.random.uniform(streams_of[3], (POSITIONS, CHAINS, BLOCK), jnp.float32) ** shard_levels(streams_of[3], (POSITIONS, CHAINS, BLOCK), ((0, 16), (1, 8)), -0.2, 0.2), 0.0, 2.0),
        "kappa": jnp.clip(0.4 + 0.6 * jax.random.uniform(streams_of[4], (POSITIONS, CHAINS, BLOCK), jnp.float32) ** shard_levels(streams_of[4], (POSITIONS, CHAINS, BLOCK), ((0, 16), (1, 8)), -0.2, 0.2), 0.4, 1.0),
        "inverse": draw_inverse(jax.random.fold_in(streams_of[8], 71), 0),
        "cell_mask": plant((jax.random.randint(streams_of[6], (POSITIONS, CHAINS, BLOCK), 0, 8) < 7).astype(jnp.int32), jax.random.fold_in(streams_of[6], 1), 0, 1),
        "upstream": draw_upstream(jax.random.fold_in(streams_of[8], 71), 0),
    }


time_step = 0.5


def reference(tile_water, tile_frac, tile_cell, storage, kappa, inverse, cell_mask, upstream):
    npos, chains, width = storage.shape
    blocks = jnp.arange(npos * chains, dtype=jnp.int32).reshape(npos, chains, 1)
    ids = (blocks * width + tile_cell).reshape(-1)
    runoff = jax.ops.segment_sum((tile_frac * tile_water).reshape(-1), ids, num_segments=npos * chains * width)
    forcing = time_step * runoff.reshape(npos, chains, width)
    mask = cell_mask.astype(jnp.float32)
    groups = (jnp.arange(chains, dtype=jnp.int32) // CH_DEV) * CH_DEV
    sources = upstream + groups[None, :]
    level = storage
    discharge = storage
    for substep in range(SUBSTEPS):
        def advance(previous, items):
            lev, force, msk, rate, matrix, src = items
            inflow = jnp.take(previous, src, axis=0)
            vector = lev + force + inflow
            wet = msk * jnp.einsum("cjk,ck->cj", matrix, vector, precision=lax.Precision.HIGHEST)
            outflow = rate * wet
            return outflow, (wet - outflow, outflow)
        start = jnp.zeros((chains, width), jnp.float32)
        _, (level, discharge) = lax.scan(advance, start, (level, forcing, mask, kappa, inverse, sources))
    return level, discharge
```

```python
import functools

import jax
import jax.numpy as jnp
from jax import lax
from jax.experimental import pallas as pl
from jax.experimental.pallas import tpu as pltpu
from jax.sharding import PartitionSpec as P

SUBSTEPS = 3

time_step = 0.5

EXTRA = 8
STORAGE, KAPPA, MASK, FORCING = 0, 1, 2, 3


def vmem():
    return pl.BlockSpec(memory_space=pltpu.VMEM)


def smem():
    return pl.BlockSpec(memory_space=pltpu.SMEM)


def runoff_kernel(water_ref, frac_ref, cell_ref, out_ref):
    rows, tiles = water_ref.shape[1:]
    half = 128
    lanes = lax.broadcasted_iota(jnp.int32, (half, tiles), 0).astype(jnp.float32).astype(jnp.bfloat16)
    one = jnp.ones((half, tiles), jnp.bfloat16)
    zero = jnp.zeros((half, tiles), jnp.bfloat16)

    def block(index, carry):
        at = pl.ds(pl.multiple_of(index * 8, 8), 8)
        value = water_ref[0, at, :] * frac_ref[0, at, :]
        cell = cell_ref[0, at, :]
        upper = cell >= half
        within = jnp.where(upper, cell - half, cell).astype(jnp.float32)
        first = value.astype(jnp.bfloat16).astype(jnp.float32)
        rest = value - first
        second = rest.astype(jnp.bfloat16).astype(jnp.float32)
        third = rest - second
        parts = []
        for piece in (first, second, third):
            parts.append(jnp.where(upper, 0.0, piece))
            parts.append(jnp.where(upper, piece, 0.0))
        outs = []
        for row in range(8):
            left = jnp.concatenate([part[row : row + 1] for part in parts] + [jnp.zeros((2, tiles), jnp.float32)], axis=0)
            owner = jnp.broadcast_to(within[row : row + 1], (half, tiles)).astype(jnp.bfloat16)
            table = jnp.where(owner == lanes, one, zero)
            sums = lax.dot_general(
                left.astype(jnp.bfloat16), table, (((1,), (1,)), ((), ())), preferred_element_type=jnp.float32
            )
            outs.append(jnp.concatenate([sums[0:1] + sums[2:3] + sums[4:5], sums[1:2] + sums[3:4] + sums[5:6]], axis=1))
        out_ref[at, :] = jnp.concatenate(outs, axis=0)
        return carry

    lax.fori_loop(0, rows // 8, block, 0)


def pack_kernel(links_ref, inverse_ref, storage_ref, kappa_ref, mask_ref, pieces_ref, packed_ref, order_ref, small_ref):
    count, rows = links_ref.shape[0], storage_ref.shape[1]
    width = storage_ref.shape[2]
    position = lax.axis_index("basin")

    def back(turn, chains):
        at = count - 1 - turn
        return tuple(links_ref[at, chain] for chain in chains)

    chains = lax.fori_loop(0, count - 1 - position, back, tuple(jnp.int32(q) for q in range(rows)))
    forcing = time_step * jnp.sum(pieces_ref[...], axis=0)
    small_ref[STORAGE] = storage_ref[0]
    small_ref[KAPPA] = kappa_ref[0]
    small_ref[MASK] = mask_ref[0].astype(jnp.float32)
    small_ref[FORCING] = forcing
    tail = jnp.zeros((EXTRA - 4, width), jnp.float32)
    for q in range(rows):
        chain = chains[q]
        packed_ref[q, 0:width, :] = inverse_ref[0, chain]
        lines = [small_ref[kind, pl.ds(chain, 1), :] for kind in range(4)]
        packed_ref[q, width : width + EXTRA, :] = jnp.concatenate(lines + [tail], axis=0)
        order_ref[q : q + 1, :] = jnp.full((1, 128), chain, jnp.int32)


def route_kernel(held_ref, out_ref):
    count = held_ref.shape[0]
    width = held_ref.shape[2]
    half = 128
    diagonal = lax.broadcasted_iota(jnp.int32, (half, half), 0) == lax.broadcasted_iota(jnp.int32, (half, half), 1)

    def turned(column):
        parts = []
        for piece in range(width // half):
            spread = jnp.where(diagonal, column[piece * half : (piece + 1) * half], 0.0)
            parts.append(jnp.sum(spread, axis=0, keepdims=True))
        return jnp.concatenate(parts, axis=1)

    def turn(t, carry):
        levels, flows = carry
        new_levels, new_flows = [], []
        for s in range(SUBSTEPS):
            p = jnp.clip(t - s, 0, count - 1)
            active = jnp.where((t >= s) & (t - s < count), 1.0, 0.0)
            line = lambda kind: held_ref[p, pl.ds(width + kind, 1), :]
            level = line(STORAGE) if s == 0 else levels[s - 1]
            vector = level + line(FORCING) + flows[s]
            column = jnp.sum(held_ref[p, 0:width, :] * vector, axis=1, keepdims=True)
            wet = active * line(MASK) * turned(column)
            flow = line(KAPPA) * wet
            new_levels.append(wet - flow)
            new_flows.append(flow)
        last = jnp.clip(t - (SUBSTEPS - 1), 0, count - 1)
        out_ref[last] = jnp.concatenate([new_levels[-1], new_flows[-1]], axis=0)
        return tuple(new_levels), tuple(new_flows)

    empty = tuple(jnp.zeros((1, width), jnp.float32) for _ in range(SUBSTEPS))
    lax.fori_loop(0, count + SUBSTEPS - 1, turn, (empty, empty))


def unpack_kernel(order_ref, result_ref, level_ref, discharge_ref):
    rows, _, width = result_ref.shape
    chain = lax.broadcasted_iota(jnp.int32, (rows, width), 0)
    level = jnp.zeros((rows, width), jnp.float32)
    discharge = jnp.zeros((rows, width), jnp.float32)
    for q in range(rows):
        mine = chain == order_ref[q : q + 1, 0:1]
        level = jnp.where(mine, result_ref[q, 0:1, :], level)
        discharge = jnp.where(mine, result_ref[q, 1:2, :], discharge)
    level_ref[0] = level
    discharge_ref[0] = discharge


def local(tile_water, tile_frac, tile_cell, storage, kappa, inverse, cell_mask, upstream):
    rows, width = storage.shape[1:]
    positions = lax.axis_size("basin")
    groups = lax.axis_size("tile")
    f32 = jnp.float32
    params = lambda mib: pltpu.CompilerParams(vmem_limit_bytes=mib << 20)

    wide = jnp.pad(upstream, ((0, 0), (0, 128 - rows)))
    links = lax.all_to_all(jnp.broadcast_to(wide, (positions, 128)), "basin", 0, 0, tiled=True)

    partial = pl.pallas_call(
        runoff_kernel,
        out_shape=jax.ShapeDtypeStruct((rows * groups, width), f32),
        in_specs=[vmem()] * 3,
        out_specs=vmem(),
        compiler_params=params(16),
        name="runoff",
    )(tile_water, tile_frac, tile_cell)
    pieces = lax.all_to_all(partial.reshape(groups, rows, width), "tile", 0, 0, tiled=True)

    packed, order = pl.pallas_call(
        pack_kernel,
        out_shape=(
            jax.ShapeDtypeStruct((rows, width + EXTRA, width), f32),
            jax.ShapeDtypeStruct((rows, 128), jnp.int32),
        ),
        in_specs=[smem()] + [vmem()] * 5,
        out_specs=(vmem(), vmem()),
        scratch_shapes=[pltpu.VMEM((4, rows, width), f32)],
        compiler_params=params(16),
        name="pack",
    )(links, inverse, storage, kappa, cell_mask, pieces)
    held = lax.all_to_all(packed, "basin", 0, 0, tiled=True)

    routed = pl.pallas_call(
        route_kernel,
        out_shape=jax.ShapeDtypeStruct((positions, 2, width), f32),
        in_specs=[vmem()],
        out_specs=vmem(),
        compiler_params=params(16),
        name="route",
    )(held)
    result = lax.all_to_all(routed, "basin", 0, 0, tiled=True)

    return pl.pallas_call(
        unpack_kernel,
        out_shape=(jax.ShapeDtypeStruct((1, rows, width), f32), jax.ShapeDtypeStruct((1, rows, width), f32)),
        in_specs=[vmem()] * 2,
        out_specs=(vmem(), vmem()),
        compiler_params=params(4),
        name="unpack",
    )(order, result)


def solution(mesh):
    placed = (
        P("basin", None, "tile"),
        P("basin", None, "tile"),
        P("basin", None, "tile"),
        P("basin", "tile", None),
        P("basin", "tile", None),
        P("basin", "tile", None, None),
        P("basin", "tile", None),
        P("basin", "tile"),
    )
    return jax.shard_map(
        local,
        mesh=mesh,
        in_specs=placed,
        out_specs=(P("basin", "tile", None), P("basin", "tile", None)),
        check_vma=False,
    )
```
